32 devices in a mesh: dp: 2 (over x), tp: 4 (over z), cp: 4 (over y, core).
Axes of the slice: x: 2, y: 2, z: 4, core: 2. Of those that a mesh axis runs over, the one named last changes fastest.
Arguments:
- x: bfloat16 [8192, 8192], P(('dp', 'cp')), parts along dimension 0
- kc: bfloat16 [16384, 8, 128], P(('dp', 'cp'), 'tp'), parts along dimension 0
- vc: bfloat16 [16384, 8, 128], P(('dp', 'cp'), 'tp'), parts along dimension 0
- wq: bfloat16 [8192, 8192], P(None, 'tp')
- wk: bfloat16 [8192, 1024], P(None, 'tp')
- wv: bfloat16 [8192, 1024], P(None, 'tp')
- wo: bfloat16 [8192, 8192], P('tp')
Outputs:
- output 1: bfloat16 [8192, 8192], P(('dp', 'cp'), 'tp'), parts along dimension 0
- output 2: bfloat16 [8192, 8, 128], P(('dp', 'cp'), 'tp'), parts along dimension 0
- output 3: bfloat16 [8192, 8, 128], P(('dp', 'cp'), 'tp'), parts along dimension 0
There are 2 independent parts. The reference program is written for one: setup_inputs(seed, part) draws one part's arguments, and reference() takes and returns one part's arrays. A program takes and returns all parts, laid end to end along the dimension named above; an argument that names none is the same for every part.
All inputs are finite; a program needn't handle non-finite values.
Results may differ from the reference program's by a relative error of at most 0.0087.
Values are sent between devices in bfloat16 or wider.
A program may use at most 1 GiB of HBM per device.

```python
import math
import jax
import jax.numpy as jnp
from jax import lax

T = 4096
C = 8192
DM = 8192
H = 64
HKV = 8
HEAD = 128
NSEG = 8
QB = 64

G = H // HKV
SCALE = HEAD ** -0.5


def _rope(a, pos):
    half = HEAD // 2
    inv = 1.0 / (500000.0 ** (jnp.arange(half, dtype=jnp.float32) * 2.0 / HEAD))
    ang = pos.astype(jnp.float32)[:, None] * inv[None, :]
    cos = jnp.cos(ang)[:, None, :]
    sin = jnp.sin(ang)[:, None, :]
    af = a.astype(jnp.float32)
    a1 = af[..., :half]
    a2 = af[..., half:]
    return jnp.concatenate([a1 * cos - a2 * sin, a2 * cos + a1 * sin], axis=-1).astype(jnp.bfloat16)


def setup_inputs(seed: int = 0, part: int = 0) -> dict:
    shared, own = jax.random.split(jax.random.key(seed))
    own = jax.random.fold_in(own, part)
    kx, kk, kv, ks, km = jax.random.split(own, 5)
    kq, kwk, kwv, kwo = jax.random.split(shared, 4)
    seg = C // NSEG
    sig = jax.random.uniform(ks, (NSEG, HKV), jnp.float32, 0.5, 1.5)
    mu = jax.random.normal(km, (NSEG, HKV, HEAD), jnp.float32)
    kc = jax.random.normal(kk, (C, HKV, HEAD), jnp.float32) * jnp.repeat(sig, seg, axis=0)[:, :, None]
    vc = jax.random.normal(kv, (C, HKV, HEAD), jnp.float32) + jnp.repeat(mu, seg, axis=0)
    x = jax.random.normal(kx, (T, DM), jnp.float32)
    gain = math.sqrt(max(1.0, 2.0 * math.log(1.2 * C / T)))
    wq = jax.random.normal(kq, (DM, H * HEAD), jnp.float32) * DM ** -0.5
    wk = jax.random.normal(kwk, (DM, HKV * HEAD), jnp.float32) * (gain * DM ** -0.5)
    wv = jax.random.normal(kwv, (DM, HKV * HEAD), jnp.float32) * DM ** -0.5
    wo = jax.random.normal(kwo, (H * HEAD, DM), jnp.float32) * (H * HEAD) ** -0.5
    bf = jnp.bfloat16
    return {'x': x.astype(bf), 'kc': kc.astype(bf), 'vc': vc.astype(bf), 'wq': wq.astype(bf),
            'wk': wk.astype(bf), 'wv': wv.astype(bf), 'wo': wo.astype(bf)}


def reference(x, kc, vc, wq, wk, wv, wo):
    f32 = jnp.float32
    pos = C + jnp.arange(T, dtype=jnp.int32)
    q = jnp.dot(x, wq, preferred_element_type=f32).astype(jnp.bfloat16).reshape(T, H, HEAD)
    k = jnp.dot(x, wk, preferred_element_type=f32).astype(jnp.bfloat16).reshape(T, HKV, HEAD)
    v = jnp.dot(x, wv, preferred_element_type=f32).astype(jnp.bfloat16).reshape(T, HKV, HEAD)
    q = _rope(q, pos).reshape(T // QB, QB, HKV, G, HEAD)
    k = _rope(k, pos)
    keys = jnp.concatenate([kc, k], axis=0).astype(f32)
    vals = jnp.concatenate([vc, v], axis=0).astype(f32)
    kpos = jnp.arange(C + T)

    def qblock(args):
        qb, i = args
        qb = qb.astype(f32)
        mask = kpos[None, :] <= (C + i * QB + jnp.arange(QB))[:, None]

        def head(j):
            s = jnp.einsum('qgd,kd->qgk', qb[:, j], keys[:, j]) * SCALE
            s = jnp.where(mask[:, None, :], s, -jnp.inf)
            p = jnp.exp(s - jnp.max(s, axis=-1, keepdims=True))
            l = jnp.sum(p, axis=-1, keepdims=True)
            o = jnp.einsum('qgk,kd->qgd', p.astype(jnp.bfloat16).astype(f32), vals[:, j])
            return o / l

        o = lax.map(head, jnp.arange(HKV))
        return o.transpose(1, 0, 2, 3).reshape(QB, H * HEAD)

    o = lax.map(qblock, (q, jnp.arange(T // QB))).reshape(T, H * HEAD)
    y = jnp.dot(o.astype(jnp.bfloat16), wo, preferred_element_type=f32).astype(jnp.bfloat16)
    return y, k, v
```

```python
import functools

import jax
import jax.numpy as jnp
from jax import lax
from jax.experimental import pallas as pl
from jax.experimental.pallas import tpu as pltpu
from jax.sharding import PartitionSpec as P

THETA = 500000.0
LOG2E = 1.4426950408889634
BK = 512
UNROLL = 8
NCHUNK = 4


def _angles(pos, d):
    half = d // 2
    inv = 1.0 / (THETA ** (jnp.arange(half, dtype=jnp.float32) * 2.0 / d))
    ang = pos.astype(jnp.float32)[:, None] * inv[None, :]
    return jnp.cos(ang), jnp.sin(ang)


def _rope(a, cos, sin):
    half = a.shape[-1] // 2
    af = a.astype(jnp.float32)
    a1, a2 = af[..., :half], af[..., half:]
    c, s = cos[:, None, :], sin[:, None, :]
    return jnp.concatenate([a1 * c - a2 * s, a2 * c + a1 * s], axis=-1).astype(jnp.bfloat16)


def _dot(a, b):
    return jnp.dot(a, b, preferred_element_type=jnp.float32)


def _attn_kernel(r_ref, q_ref, cos_ref, sin_ref, k_ref, vt_ref, o_ref,
                 s_scr, mx_scr, qt_scr, acc, m_scr, l_scr, *, ncache, tl, scale2):
    bq, d = q_ref.shape
    r = r_ref[0]
    nb = tl // BK
    nc = ncache // BK
    q = q_ref[...].astype(jnp.float32)
    q = q * cos_ref[...] + pltpu.roll(q, d // 2, 1) * sin_ref[...]
    qt_scr[...] = q.astype(jnp.bfloat16).T
    m_scr[...] = jnp.full_like(m_scr, -jnp.inf)
    l_scr[...] = jnp.zeros_like(l_scr)
    acc[...] = jnp.zeros_like(acc)

    def offset(i):
        n = i - nc
        new = ncache + ((n // nb) ^ r) * tl + (n % nb) * BK
        return pl.multiple_of(jnp.where(i < nc, i * BK, new), BK)

    def visible(part):
        key = lax.broadcasted_iota(jnp.int32, (BK, bq), 0) + part * BK
        return key <= lax.broadcasted_iota(jnp.int32, (BK, bq), 1)

    def scores(off, slot, part=None):
        s = _dot(k_ref[pl.ds(off, BK), :], qt_scr[...])
        if part is not None:
            s = jnp.where(visible(part), s, -jnp.inf)
        s_scr[slot] = s
        mx_scr[slot] = jnp.max(s, axis=0, keepdims=True)

    def update(off, slot, part=None):
        s = s_scr[slot]
        mx = mx_scr[slot]
        if part is not None:
            s = jnp.where(visible(part), s, -jnp.inf)
            mx = jnp.max(s, axis=0, keepdims=True)
        mo = m_scr[...]
        mn = jnp.maximum(mo, mx)
        p = jnp.exp2((s - mn) * scale2)
        a = jnp.exp2((mo - mn) * scale2)
        l_scr[...] = l_scr[...] * a + jnp.sum(p, axis=0, keepdims=True)
        m_scr[...] = mn
        acc[...] = acc[...] * a + _dot(vt_ref[:, pl.ds(off, BK)], p.astype(jnp.bfloat16))

    scores(0, 0)

    def cache_step(j, carry):
        for u in range(UNROLL):
            i = j * UNROLL + u
            scores(offset(i + 1), (u + 1) % 2)
            update(pl.multiple_of(i * BK, BK), u % 2)
        return carry

    lax.fori_loop(0, nc // UNROLL, cache_step, 0)

    def new_step(j, carry):
        for u in range(nb):
            i = nc + j * nb + u
            scores(offset(i + 1), (u + 1) % 2)
            update(offset(i), u % 2)
        return carry

    lax.fori_loop(0, r, new_step, 0)
    for part in range(nb):
        if part < nb - 1:
            scores(ncache + (part + 1) * BK, (part + 1) % 2, part + 1)
        update(ncache + part * BK, part % 2, part if part == 0 else None)
    o_ref[...] = (acc[...] / l_scr[...]).T.astype(jnp.bfloat16)


def _attend(r, q, cos, sin, k, vt, *, first, heads, group, ncache):
    tl = q.shape[0]
    d = k.shape[-1]
    total = k.shape[1]
    kv = first // group
    est = pl.CostEstimate(flops=heads * tl * 10240 * d * 10, transcendentals=heads * tl * 10240,
                          bytes_accessed=4 * total * d + 4 * heads * tl * d)
    return pl.pallas_call(
        functools.partial(_attn_kernel, ncache=ncache, tl=tl, scale2=d ** -0.5 * LOG2E),
        grid_spec=pltpu.PrefetchScalarGridSpec(
            num_scalar_prefetch=1, grid=(heads,),
            in_specs=[pl.BlockSpec((tl, d), lambda h, r: (0, first + h)),
                      pl.BlockSpec((tl, d), lambda h, r: (0, 0)),
                      pl.BlockSpec((tl, d), lambda h, r: (0, 0)),
                      pl.BlockSpec((None, total, d), lambda h, r: (kv, 0, 0)),
                      pl.BlockSpec((None, d, total), lambda h, r: (kv, 0, 0))],
            out_specs=pl.BlockSpec((tl, d), lambda h, r: (0, h)),
            scratch_shapes=[pltpu.VMEM((2, BK, tl), jnp.float32), pltpu.VMEM((2, 1, tl), jnp.float32),
                            pltpu.VMEM((d, tl), jnp.bfloat16), pltpu.VMEM((d, tl), jnp.float32),
                            pltpu.VMEM((1, tl), jnp.float32), pltpu.VMEM((1, tl), jnp.float32)]),
        out_shape=jax.ShapeDtypeStruct((tl, heads * d), jnp.bfloat16),
        compiler_params=pltpu.CompilerParams(vmem_limit_bytes=56 * 2 ** 20, dimension_semantics=("arbitrary",)),
        cost_estimate=est,
    )(r, q, cos, sin, k, vt)


def _out_kernel(idx_ref, *refs, nchunks, has_init):
    o_refs = refs[:nchunks]
    own_ref, mate_ref, local_ref = refs[nchunks:nchunks + 3]
    init_ref = refs[nchunks + 3] if has_init else None
    y_ref, acc = refs[-2:]
    n, c, s = pl.program_id(0), pl.program_id(1), pl.program_id(2)
    core = idx_ref[0]
    sl = own_ref.shape[-2]

    @pl.when((c == 0) & (s == 0))
    def _():
        acc[...] = init_ref[...] if has_init else jnp.zeros_like(acc)

    for cc in range(nchunks):
        @pl.when((c == cc) & (s == 3))
        def _(cc=cc):
            acc[...] += _dot(o_refs[cc][...], local_ref[...])

        @pl.when((c == cc) & (s < 3))
        def _(cc=cc):
            a = o_refs[cc][:, pl.ds(pl.multiple_of(core * sl, 128), sl)]
            b = o_refs[cc][:, pl.ds(pl.multiple_of((1 - core) * sl, 128), sl)]
            acc[...] += _dot(a, own_ref[...]) + _dot(b, mate_ref[...])

    @pl.when((c == nchunks - 1) & (s == 3))
    def _():
        y_ref[...] = acc[...].astype(y_ref.dtype)


def _project_out(idx, os, own, mate, wo, init, *, chunks, dtype):
    rows, width = os[0].shape[1:]
    sl, nh = own.shape[-2:]
    nc = len(chunks)
    c0 = chunks[0]

    def o_map(cc):
        def f(n, c, s, i):
            t = jnp.where(c < cc, 0, jnp.where(c > cc, 3, s))
            return ((i[3] + 3 - t) % 4, 0, 0)
        return f

    def p_map(n, c, s, i):
        c = c + c0
        slot = ((c % 2) ^ i[2]) * 2 + ((c // 2) ^ i[1])
        return (n, slot, jnp.minimum(s, 2), 0, 0)

    in_specs = [pl.BlockSpec((None, rows, width), o_map(cc)) for cc in range(nc)]
    in_specs += [pl.BlockSpec((None, None, None, sl, nh), p_map)] * 2
    in_specs += [pl.BlockSpec((width, nh), lambda n, c, s, i: (c + c0, i[3] * 2 + n))]
    args = list(os) + [own, mate, wo]
    if init is not None:
        in_specs.append(pl.BlockSpec((rows, nh), lambda n, c, s, i: (0, n)))
        args.append(init)
    flops = 2 * rows * width * 4 * nc * nh * 2
    return pl.pallas_call(
        functools.partial(_out_kernel, nchunks=nc, has_init=init is not None),
        grid_spec=pltpu.PrefetchScalarGridSpec(
            num_scalar_prefetch=1, grid=(2, nc, 4), in_specs=in_specs,
            out_specs=pl.BlockSpec((rows, nh), lambda n, c, s, i: (0, n)),
            scratch_shapes=[pltpu.VMEM((rows, nh), jnp.float32)]),
        out_shape=jax.ShapeDtypeStruct((rows, 2 * nh), dtype),
        compiler_params=pltpu.CompilerParams(vmem_limit_bytes=60 * 2 ** 20,
                                             dimension_semantics=("arbitrary",) * 3),
        cost_estimate=pl.CostEstimate(flops=flops, transcendentals=0, bytes_accessed=flops // 512),
    )(idx, *args)


def solution(mesh):
    ncp = mesh.shape['cp']
    ntp = mesh.shape['tp']
    row = P(('dp', 'cp'), None)
    cache = P(('dp', 'cp'), 'tp', None)
    col = P(None, 'tp')
    swap_core = [(i, i ^ 1) for i in range(4)]
    swap_y = [(i, i ^ 2) for i in range(4)]
    swap_x = [(0, 1), (1, 0)]

    def over_core(a):
        return lax.ppermute(a, 'cp', swap_core)

    def over_y(a):
        return lax.ppermute(a, 'cp', swap_y)

    def over_x(a):
        return lax.ppermute(a, 'dp', swap_x)

    def body(x, kc, vc, wq, wk, wv, wo):
        tl, dm = x.shape
        cl, hkvl, d = kc.shape
        hl = wq.shape[1] // d
        g = hl // hkvl
        dp, tp, r = lax.axis_index('dp'), lax.axis_index('tp'), lax.axis_index('cp')
        y_, core = r // 2, r % 2

        def spread(a):
            b = over_y(a)
            return [a, over_core(a), b, over_core(b)]

        kt = spread(kc.transpose(1, 0, 2))
        vt = spread(vc.transpose(1, 2, 0))

        sl = hl * d // 8
        nh = dm // ntp // 2
        me = dp * 4 + r
        rows = lax.dynamic_slice_in_dim(wo, me * sl, sl, axis=0)
        got = []
        for s in range(1, ntp):
            dst = (tp + s) % ntp
            piece = lax.dynamic_slice_in_dim(rows, dst * (2 * nh), 2 * nh, axis=1)
            got.append(lax.ppermute(piece, 'tp', [(i, (i + s) % ntp) for i in range(ntp)]))
        got = jnp.stack(got)
        pa, pb = got[..., :nh], got[..., nh:]
        pa = jnp.stack([pa, over_x(pa)])
        pb = jnp.stack([pb, over_y(pb)])
        pa = jnp.stack([pa, over_y(pa)])
        pb = jnp.stack([pb, over_x(pb)], axis=1)
        own = jnp.stack([pa, pb]).reshape(2, 4, ntp - 1, sl, nh)
        mate = over_core(own)

        pos = cl * ncp + r * tl + jnp.arange(tl, dtype=jnp.int32)
        cos, sin = _angles(pos, d)
        k = _dot(x, wk).astype(jnp.bfloat16).reshape(tl, hkvl, d)
        k = _rope(k, cos, sin)
        v = _dot(x, wv).astype(jnp.bfloat16).reshape(tl, hkvl, d)
        kt += spread(k.transpose(1, 0, 2))
        vt += spread(v.transpose(1, 2, 0))
        q = _dot(x, wq).astype(jnp.bfloat16)
        k_all = jnp.concatenate(kt, axis=1)
        vt_all = jnp.concatenate(vt, axis=2)
        cos2 = jnp.concatenate([cos, cos], axis=1)
        sin2 = jnp.concatenate([-sin, sin], axis=1)

        heads = hl // NCHUNK
        rr = r.reshape(1).astype(jnp.int32)
        os = []
        for c in range(NCHUNK):
            o = _attend(rr, q, cos2, sin2, k_all, vt_all, first=c * heads, heads=heads, group=g,
                        ncache=cl * ncp)
            os.append(lax.all_gather(o, 'tp', axis=0, tiled=False))
        idx = jnp.stack([core, dp, y_, tp]).astype(jnp.int32)
        part = _project_out(idx, os[:-1], own, mate, wo, None, chunks=list(range(NCHUNK - 1)),
                            dtype=jnp.float32)
        y = _project_out(idx, os[-1:], own, mate, wo, part, chunks=[NCHUNK - 1], dtype=jnp.bfloat16)
        return y, k, v

    return jax.shard_map(body, mesh=mesh,
                         in_specs=(row, cache, cache, col, col, col, P('tp', None)),
                         out_specs=(P(('dp', 'cp'), 'tp'), cache, cache), check_vma=False)
```

```python
import functools

import jax
import jax.numpy as jnp
from jax import lax
from jax.experimental import pallas as pl
from jax.experimental.pallas import tpu as pltpu
from jax.sharding import PartitionSpec as P


THETA = 500000.0
LOG2E = 1.4426950408889634
BK = 512
KC = 1024
UNROLL = 2
NCHUNK = 4
SPLIT = 2


def _angles(pos, d):
    half = d // 2
    inv = 1.0 / (THETA ** (jnp.arange(half, dtype=jnp.float32) * 2.0 / d))
    ang = pos.astype(jnp.float32)[:, None] * inv[None, :]
    return jnp.cos(ang), jnp.sin(ang)


def _rope(a, cos, sin):
    half = a.shape[-1] // 2
    af = a.astype(jnp.float32)
    a1, a2 = af[..., :half], af[..., half:]
    c, s = cos[:, None, :], sin[:, None, :]
    return jnp.concatenate([a1 * c - a2 * s, a2 * c + a1 * s], axis=-1).astype(jnp.bfloat16)


def _dot(a, b):
    return jnp.dot(a, b, preferred_element_type=jnp.float32)


def _attn_kernel(r_ref, q_ref, cos_ref, sin_ref, *refs, ncache, tl, scale2, nblk):
    kc_refs, vc_refs, kn_refs, vn_refs = (refs[i * nblk:(i + 1) * nblk] for i in range(4))
    o_ref, k_ref, vt_ref, s_scr, mx_scr, qt_scr, acc, m_scr, l_scr = refs[4 * nblk:]
    bq, d = q_ref.shape
    cl = ncache // nblk

    @pl.when(pl.program_id(0) == 0)
    def _():
        for i in range(nblk):
            k_ref[i * cl:(i + 1) * cl, :] = kc_refs[i][...]
            vt_ref[:, i * cl:(i + 1) * cl] = vc_refs[i][...]
            k_ref[ncache + i * tl:ncache + (i + 1) * tl, :] = kn_refs[i][...]
            vt_ref[:, ncache + i * tl:ncache + (i + 1) * tl] = vn_refs[i][...]

    r = r_ref[0]
    nb = tl // BK
    nc = ncache // BK
    q = q_ref[...].astype(jnp.float32)
    q = q * cos_ref[...] + pltpu.roll(q, d // 2, 1) * sin_ref[...]
    qt_scr[...] = q.astype(jnp.bfloat16).T
    m_scr[...] = jnp.full_like(m_scr, -jnp.inf)
    l_scr[...] = jnp.zeros_like(l_scr)
    acc[...] = jnp.zeros_like(acc)

    def offset(i):
        n = i - nc
        new = ncache + ((n // nb) ^ r) * tl + (n % nb) * BK
        return pl.multiple_of(jnp.where(i < nc, i * BK, new), BK)

    def visible(part):
        key = lax.broadcasted_iota(jnp.int32, (BK, bq), 0) + part * BK
        return key <= lax.broadcasted_iota(jnp.int32, (BK, bq), 1)

    def scores(off, slot, size=BK, part=None):
        s = _dot(k_ref[pl.ds(off, size), :], qt_scr[...])
        if part is not None:
            s = jnp.where(visible(part), s, -jnp.inf)
        s_scr[slot, :size, :] = s
        mx_scr[slot] = jnp.max(s, axis=0, keepdims=True)

    def update(off, slot, size=BK, part=None):
        s = s_scr[slot, :size, :]
        mx = mx_scr[slot]
        if part is not None:
            s = jnp.where(visible(part), s, -jnp.inf)
            mx = jnp.max(s, axis=0, keepdims=True)
        mo = m_scr[...]
        mn = jnp.maximum(mo, mx)
        p = jnp.exp2((s - mn) * scale2)
        a = jnp.exp2((mo - mn) * scale2)
        l_scr[...] = l_scr[...] * a + jnp.sum(p, axis=0, keepdims=True)
        m_scr[...] = mn
        acc[...] = acc[...] * a + _dot(vt_ref[:, pl.ds(off, size)], p.astype(jnp.bfloat16))

    scores(0, 0, KC)
    ncc = ncache // KC

    def cache_steps(base, last):
        for u in range(UNROLL):
            i = base + u
            if last and u == UNROLL - 1:
                scores(offset(nc), 0)
            else:
                scores(pl.multiple_of((i + 1) * KC, KC), (u + 1) % 2, KC)
            update(pl.multiple_of(i * KC, KC), u % 2, KC)

    def cache_step(j, carry):
        cache_steps(j * UNROLL, False)
        return carry

    lax.fori_loop(0, ncc // UNROLL - 1, cache_step, 0)
    cache_steps(jnp.int32(ncc - UNROLL), True)

    def new_step(j, carry):
        for u in range(nb):
            i = nc + j * nb + u
            scores(offset(i + 1), (u + 1) % 2)
            update(offset(i), u % 2)
        return carry

    lax.fori_loop(0, r, new_step, 0)
    for part in range(nb):
        if part < nb - 1:
            scores(ncache + (part + 1) * BK, (part + 1) % 2, part=part + 1)
        update(ncache + part * BK, part % 2, part=part if part == 0 else None)
    o_ref[...] = (acc[...] / l_scr[...]).T.astype(jnp.bfloat16)


def _attend(r, q, cos, sin, kc, vc, kn, vn, *, first, heads, group):
    tl = q.shape[0]
    nblk = len(kc)
    _, cl, d = kc[0].shape
    ncache = nblk * cl
    total = ncache + nblk * tl
    kv = first // group
    est = pl.CostEstimate(flops=heads * tl * 10240 * d * 10, transcendentals=heads * tl * 10240,
                          bytes_accessed=4 * total * d + 4 * heads * tl * d)
    blocks = list(kc) + list(vc) + list(kn) + list(vn)
    return pl.pallas_call(
        functools.partial(_attn_kernel, ncache=ncache, tl=tl, scale2=d ** -0.5 * LOG2E, nblk=nblk),
        grid_spec=pltpu.PrefetchScalarGridSpec(
            num_scalar_prefetch=1, grid=(heads,),
            in_specs=[pl.BlockSpec((tl, d), lambda h, r: (0, first + h)),
                      pl.BlockSpec((tl, d), lambda h, r: (0, 0)),
                      pl.BlockSpec((tl, d), lambda h, r: (0, 0))]
            + [pl.BlockSpec((None,) + a.shape[1:], lambda h, r: (kv, 0, 0)) for a in blocks],
            out_specs=pl.BlockSpec((tl, d), lambda h, r: (0, h)),
            scratch_shapes=[pltpu.VMEM((total, d), jnp.bfloat16), pltpu.VMEM((d, total), jnp.bfloat16),
                            pltpu.VMEM((2, KC, tl), jnp.float32), pltpu.VMEM((2, 1, tl), jnp.float32),
                            pltpu.VMEM((d, tl), jnp.bfloat16), pltpu.VMEM((d, tl), jnp.float32),
                            pltpu.VMEM((1, tl), jnp.float32), pltpu.VMEM((1, tl), jnp.float32)]),
        out_shape=jax.ShapeDtypeStruct((tl, heads * d), jnp.bfloat16),
        compiler_params=pltpu.CompilerParams(vmem_limit_bytes=56 * 2 ** 20, dimension_semantics=("arbitrary",)),
        cost_estimate=est,
    )(r, q, cos, sin, *blocks)


def _out_kernel(idx_ref, *refs, parts, has_init):
    refs = list(refs)
    y_ref = refs.pop()
    init_ref = refs.pop() if has_init else None
    core, z = idx_ref[0], idx_ref[3]
    in_a = pl.program_id(0) < pl.num_programs(0) // 2
    total = init_ref[...] if has_init else None
    for npart in parts:
        o_refs, (own_a, own_b, mate_a, mate_b, local_ref) = refs[:npart], refs[npart:npart + 5]
        refs = refs[npart + 5:]
        sl = own_a.shape[-2]
        lhs, rhs = [], []
        for s in range(3):
            t = (z + 3 - s) % 4
            if npart == 1:
                a = o_refs[0][t, :, pl.ds(pl.multiple_of(core * sl, 128), sl)]
                b = o_refs[0][t, :, pl.ds(pl.multiple_of((1 - core) * sl, 128), sl)]
            else:
                lo, hi = o_refs[0][t], o_refs[1][t]
                a, b = jnp.where(core == 0, lo, hi), jnp.where(core == 0, hi, lo)
            lhs += [a, b]
            rhs += [jnp.where(in_a, own_a[s], own_b[s]), jnp.where(in_a, mate_a[s], mate_b[s])]
        lhs += [o[z] for o in o_refs]
        rhs += [local_ref[...]]
        p = _dot(jnp.concatenate(lhs, axis=1), jnp.concatenate(rhs, axis=0))
        total = p if total is None else total + p
    y_ref[...] = total.astype(y_ref.dtype)


def _project_out(idx, os, own, mate, wo, init, *, chunks, dtype, nt=512):
    rows = os[0][0].shape[1]
    sl, nh = own[0].shape[-2:]
    ncols = 2 * nh
    per = nh // nt

    def p_map(c, b):
        def f(n, i):
            n = jnp.maximum(n - per, 0) if b else jnp.minimum(n, per - 1)
            return (((c % 2) ^ i[2]) * 2 + ((c // 2) ^ i[1]), 0, 0, n)

        return f

    def l_map(c):
        return lambda n, i: (c, i[3] * (ncols // nt) + n)

    in_specs, args = [], []
    for c, parts in zip(chunks, os):
        in_specs += [pl.BlockSpec(o.shape, lambda n, i: (0, 0, 0)) for o in parts]
        in_specs += [pl.BlockSpec((None, 3, sl, nt), p_map(c, b)) for b in (0, 1)] * 2
        in_specs += [pl.BlockSpec((2 * sl, nt), l_map(c))]
        args += list(parts) + [*own, *mate, wo]
    if init is not None:
        in_specs.append(pl.BlockSpec((rows, nt), lambda n, i: (0, n)))
        args.append(init)
    flops = 2 * rows * 2 * sl * 4 * len(chunks) * ncols
    return pl.pallas_call(
        functools.partial(_out_kernel, parts=[len(p) for p in os], has_init=init is not None),
        grid_spec=pltpu.PrefetchScalarGridSpec(
            num_scalar_prefetch=1, grid=(ncols // nt,), in_specs=in_specs,
            out_specs=pl.BlockSpec((rows, nt), lambda n, i: (0, n))),
        out_shape=jax.ShapeDtypeStruct((rows, ncols), dtype),
        compiler_params=pltpu.CompilerParams(vmem_limit_bytes=60 * 2 ** 20,
                                             dimension_semantics=("arbitrary",)),
        cost_estimate=pl.CostEstimate(flops=flops, transcendentals=0, bytes_accessed=flops // 512),
    )(idx, *args)


def solution(mesh):
    ncp = mesh.shape['cp']
    ntp = mesh.shape['tp']
    row = P(('dp', 'cp'), None)
    cache = P(('dp', 'cp'), 'tp', None)
    col = P(None, 'tp')
    swap_core = [(i, i ^ 1) for i in range(4)]
    swap_y = [(i, i ^ 2) for i in range(4)]
    swap_x = [(0, 1), (1, 0)]

    def over_core(a):
        return lax.ppermute(a, 'cp', swap_core)

    def over_y(a):
        return lax.ppermute(a, 'cp', swap_y)

    def over_x(a):
        return lax.ppermute(a, 'dp', swap_x)

    def body(x, kc, vc, wq, wk, wv, wo):
        tl, dm = x.shape
        cl, hkvl, d = kc.shape
        hl = wq.shape[1] // d
        g = hl // hkvl
        dp, tp, r = lax.axis_index('dp'), lax.axis_index('tp'), lax.axis_index('cp')
        y_, core = r // 2, r % 2

        sl = hl * d // 8
        nh = dm // ntp // 2
        me = dp * 4 + r
        kct, vct = kc.transpose(1, 0, 2), vc.transpose(1, 2, 0)
        far = [over_y(kct), over_y(vct)]
        pos = cl * ncp + r * tl + jnp.arange(tl, dtype=jnp.int32)
        cos, sin = _angles(pos, d)
        wkv = jnp.concatenate([wk, wv], axis=1)
        kv = _dot(x, wkv).astype(jnp.bfloat16)
        k = _rope(kv[:, :hkvl * d].reshape(tl, hkvl, d), cos, sin)
        v = kv[:, hkvl * d:].reshape(tl, hkvl, d)
        knt, vnt = k.transpose(1, 0, 2), v.transpose(1, 2, 0)
        far += [over_y(knt), over_y(vnt)]

        rows = lax.dynamic_slice_in_dim(wo, me * sl, sl, axis=0)
        got = []
        for s in range(1, ntp):
            dst = (tp + s) % ntp
            piece = lax.dynamic_slice_in_dim(rows, dst * (2 * nh), 2 * nh, axis=1)
            got.append(lax.ppermute(piece, 'tp', [(i, (i + s) % ntp) for i in range(ntp)]))
        q = _dot(x, wq).astype(jnp.bfloat16)
        near = [kct, vct, knt, vnt]
        far, q = lax.optimization_barrier((far, q))
        kcs, vcs, kns, vns = ([a, over_core(a), b, over_core(b)] for a, b in zip(near, far))

        cos2 = jnp.concatenate([cos, cos], axis=1)
        sin2 = jnp.concatenate([-sin, sin], axis=1)
        heads = hl // NCHUNK
        rr = r.reshape(1).astype(jnp.int32)

        def attend(first, n):
            o = _attend(rr, q, cos2, sin2, kcs, vcs, kns, vns, first=first, heads=n, group=g)
            return o

        def gather(o):
            return lax.all_gather(o, 'tp', axis=0, tiled=False)

        half = heads // 2
        os = []
        for c in range(NCHUNK):
            n = half if c < SPLIT else heads
            os.append([attend(first, n) for first in range(c * heads, (c + 1) * heads, n)])
        head0, head1 = os[0][0], os[-2][-1]
        os = [tuple(gather(o) for o in parts) for parts in os]

        got, _ = lax.optimization_barrier((got, head0))
        got = jnp.stack(got)
        pa, pb = got[..., :nh], got[..., nh:]
        pa = jnp.stack([pa, over_x(pa)])
        pb = jnp.stack([pb, over_y(pb)])
        pa = jnp.stack([pa, over_y(pa)])
        pb = jnp.stack([pb, over_x(pb)], axis=1)
        own = [a.reshape(4, ntp - 1, sl, nh) for a in (pa, pb)]
        own, _ = lax.optimization_barrier((own, head1))
        mate = [over_core(a) for a in own]
        idx = jnp.stack([core, dp, y_, tp]).astype(jnp.int32)
        part = _project_out(idx, os[:-1], own, mate, wo, None, chunks=list(range(NCHUNK - 1)),
                            dtype=jnp.float32)
        y = _project_out(idx, os[-1:], own, mate, wo, part, chunks=[NCHUNK - 1], dtype=jnp.bfloat16)
        return y, k, v

    return jax.shard_map(body, mesh=mesh,
                         in_specs=(row, cache, cache, col, col, col, P('tp', None)),
                         out_specs=(P(('dp', 'cp'), 'tp'), cache, cache), check_vma=False)
```
